128 devices in a mesh: dp: 8 (over z_hi, y), tensor: 16 (over z_lo, x, core).
Axes of the slice: x: 4, y: 4, z: 4 (z_hi: 2, z_lo: 2; z = z_hi * 2 + z_lo), core: 2. Of those that a mesh axis runs over, the one named last changes fastest.
Arguments:
- normed_input: bfloat16 [8192, 8192], P('dp', 'tensor'), may hold values from -6 to 6
- positions: int32 [8192], P('dp'), may hold values from 0 to 8191
- fixed_weight_matrix: bfloat16 [8192, 10240], P('dp', 'tensor'), may hold values from -0.09375 to 0.09375
- adapter_down_map: bfloat16 [8192, 16], P('tensor'), may hold values from -0.0625 to 0.0625
- adapter_up_map: bfloat16 [16, 10240], P(None, 'tensor'), may hold values from -0.0625 to 0.0625
- output_gradient: bfloat16 [8192, 10240], P('dp', 'tensor'), may hold values from -6 to 6
Outputs:
- grad_x: bfloat16 [8192, 8192], P('dp', 'tensor')
- grad_a: float32 [8192, 16], P('tensor')
- grad_b: float32 [16, 10240], P(None, 'tensor')
The draws below stay inside these ranges and needn't reach their ends.
All inputs are finite; a program needn't handle non-finite values.
Results may differ from the reference program's by a relative error of at most 0.0048.
Values may be sent and summed in bfloat16 or wider, within the bound.
No kernel may reach another device: no remote copies, remote signals or barrier semaphores. Data moves between devices by JAX's collectives and lax.ppermute only.
A program may use at most 256 MiB of HBM per device.

```python
import jax
import jax.numpy as jnp

MODEL_WIDTH = 8192
KV = 1024
HEAD = 128
ADAPTER_RANK = 16
PROJECTION_COLS = 10240
TOKENS = 8192
N_TENSOR = 16


def place_ends(entries, stream_key, low, largest):
    index_at = [jax.random.randint(jax.random.fold_in(stream_key, axis), (), 0, length) for axis, length in enumerate(entries.shape)]
    longest = entries.shape.index(max(entries.shape))
    neighbour = index_at[:longest] + [(index_at[longest] + 1) % entries.shape[longest]] + index_at[longest + 1:]
    return entries.at[tuple(index_at)].set(low).at[tuple(neighbour)].set(largest)


def strengthened(array, rng, source, target, blocks, factor):
    owner, partner = [(jnp.arange(array.shape[dim]) // (array.shape[dim] // blocks)).reshape([-1 if axis == dim else 1 for axis in range(array.ndim)]) for dim in (source, target)]
    chosen = jax.random.permutation(rng, blocks)[partner]
    strong = (owner == chosen) | (owner == (partner + blocks // 2) % blocks)
    return jnp.where(strong, factor * array, array)


def shard_levels(key, extent, split, low, high):
    gain = 1.0
    for position, shards_of in split:
        heights = jax.random.uniform(jax.random.fold_in(jax.random.fold_in(key, 6), position), (shards_of,), jnp.float32, low / len(split), high / len(split))
        gain = gain * jnp.repeat(jnp.exp(heights), extent[position] // shards_of).reshape((-1,) + (1,) * (len(extent) - 1 - position))
    return gain


def gaussian(rng, dims, deviation, bound, pieces=(), kind=jnp.bfloat16):
    values = deviation * jax.random.normal(rng, dims, jnp.float32)
    if pieces:
        values = values * shard_levels(rng, dims, pieces, -0.22, 0.18)
    return jnp.clip(values, -bound, bound).astype(kind)


def noise_with(key, extent, scale, most, pieces, heavy, kind=jnp.bfloat16):
    entries = scale * jax.random.normal(key, extent, jnp.float32)
    if pieces:
        entries = entries * shard_levels(key, extent, pieces, -0.22, 0.18)
    return jnp.clip(strengthened(entries, jax.random.fold_in(key, 3), *heavy), -most, most).astype(kind)


def setup_inputs(seed: int = 0) -> dict:
    streams_of = jax.random.split(jax.random.key(seed), 7)
    return {
        "normed_input": gaussian(streams_of[0], (TOKENS, MODEL_WIDTH), 1.0, 6.0, ((0, 8), (1, 16))),
        "positions": place_ends(jax.random.randint(streams_of[1], (TOKENS,), 0, TOKENS), jax.random.fold_in(streams_of[1], 1), 0, TOKENS - 1).astype(jnp.int32),
        "fixed_weight_matrix": noise_with(streams_of[2], (MODEL_WIDTH, PROJECTION_COLS), MODEL_WIDTH ** -0.5, 0.09375, ((0, 8), (1, 16)), (1, 0, 16, 2.0)),
        "adapter_down_map": gaussian(streams_of[3], (MODEL_WIDTH, ADAPTER_RANK), MODEL_WIDTH ** -0.5, 0.0625, ((0, 16),)),
        "adapter_up_map": gaussian(streams_of[4], (ADAPTER_RANK, PROJECTION_COLS), PROJECTION_COLS ** -0.5, 0.0625, ((1, 16),)),
        "output_gradient": gaussian(streams_of[5], (TOKENS, PROJECTION_COLS), 1.0, 6.0, ((0, 8), (1, 16))),
    }


def rope_tables(positions, qkv):
    width = qkv // N_TENSOR
    q_width = MODEL_WIDTH // N_TENSOR
    k_width = KV // N_TENSOR
    column = jnp.arange(qkv, dtype=jnp.int32)
    block = column // width
    offset = column % width
    is_query = offset < q_width
    is_key = jnp.logical_and(offset >= q_width, offset < q_width + k_width)
    dimension = jnp.where(is_query, (block * q_width + offset) % HEAD, (block * k_width + offset - q_width) % HEAD)
    pair = (dimension // 2).astype(jnp.float32)
    freq = jnp.float32(500000.0) ** (-2.0 * pair / HEAD)
    angle = positions.astype(jnp.float32)[:, None] * freq[None, :]
    rotate = jnp.logical_or(is_query, is_key)[None, :]
    cosine = jnp.where(rotate, jnp.cos(angle), jnp.float32(1.0))
    sine = jnp.where(rotate, jnp.sin(angle), jnp.float32(0.0))
    return cosine[:, 0::2], sine[:, 0::2]


def reference(normed_input, positions, fixed_weight_matrix, adapter_down_map, adapter_up_map, output_gradient):
    rows, qkv = output_gradient.shape
    cosine, sine = rope_tables(positions, qkv)
    pairs = output_gradient.astype(jnp.float32).reshape(rows, qkv // 2, 2)
    first = pairs[:, :, 0] * cosine + pairs[:, :, 1] * sine
    second = pairs[:, :, 1] * cosine - pairs[:, :, 0] * sine
    unrotated_gradient = jnp.stack([first, second], axis=2).reshape(rows, qkv).astype(jnp.bfloat16)
    rank_input = jnp.dot(normed_input, adapter_down_map, preferred_element_type=jnp.float32)
    rank_gradient = jnp.dot(unrotated_gradient, adapter_up_map.T, preferred_element_type=jnp.float32)
    low_xb = rank_input.astype(jnp.bfloat16)
    rank_gradient_up = rank_gradient.astype(jnp.bfloat16)
    base = jnp.dot(unrotated_gradient, fixed_weight_matrix.T, preferred_element_type=jnp.float32)
    adapter_branch = jnp.dot(rank_gradient_up, adapter_down_map.T, preferred_element_type=jnp.float32)
    grad_x = (base + 2.0 * adapter_branch).astype(jnp.bfloat16)
    factor = 2.0 / (float(TOKENS) ** 0.5)
    grad_a = factor * jnp.dot(normed_input.T, rank_gradient_up, preferred_element_type=jnp.float32)
    grad_b = factor * jnp.dot(low_xb.T, unrotated_gradient, preferred_element_type=jnp.float32)
    return grad_x, grad_a, grad_b
```

```python
import functools
import math

import jax
import jax.numpy as jnp
from jax import lax
from jax.experimental import pallas as pl
from jax.experimental.pallas import tpu as pltpu
from jax.sharding import PartitionSpec as P

HEAD = 128
Q_SHARD = 512
K_SHARD = 64
RANK = 16
AXES = ("dp", "tensor")
BF16 = jnp.bfloat16
F32 = jnp.float32


def number(x, y, z, k):
    return ((z // 2) * 4 + y) * 16 + (z % 2) * 8 + x * 2 + k


CHIPS = [(x, y, z, k) for x in range(4) for y in range(4) for z in range(4) for k in range(2)]


def send(value, dx=0, dy=0, dk=0, zx=0, xx=0, yx=0, zmap=None):
    pairs = []
    for x, y, z, k in CHIPS:
        if zmap is None:
            to = z ^ zx
        elif z in zmap:
            to = zmap[z]
        else:
            continue
        pairs.append(
            (number(x, y, z, k), number(((x + dx) % 4) ^ xx, ((y + dy) % 4) ^ yx, to, k ^ dk))
        )
    return lax.ppermute(value, AXES, pairs)


def nt(a, b):
    return lax.dot_general(a, b, (((1,), (1,)), ((), ())), preferred_element_type=F32)


def rotate_kernel(odd_ref, g_ref, cos_ref, sin_ref, swap_ref, x_ref, down_ref, up_ref, y_ref, low_ref):
    cosine = cos_ref[...]
    sine = sin_ref[...]
    odd = odd_ref[0] == 1
    lane = lax.broadcasted_iota(jnp.int32, cosine.shape, 1)
    key_cos = jnp.where(odd, pltpu.roll(cosine, 64, 1), cosine)
    key_sin = jnp.where(odd, pltpu.roll(sine, 64, 1), sine)
    key_cos = jnp.where(lane < K_SHARD, key_cos, 1.0)
    key_sin = jnp.where(lane < K_SHARD, key_sin, 0.0)
    groups = g_ref.shape[1] // HEAD
    for i in range(groups):
        g = g_ref[:, i * HEAD : (i + 1) * HEAD]
        turned = jnp.dot(g, swap_ref[...], preferred_element_type=F32)
        c = cosine if i < groups - 1 else key_cos
        s = sine if i < groups - 1 else key_sin
        y_ref[:, i * HEAD : (i + 1) * HEAD] = (g.astype(F32) * c + turned * s).astype(BF16)
    low_ref[:RANK, :] = nt(down_ref[...], x_ref[...])
    low_ref[RANK:, :] = nt(up_ref[...], y_ref[...])


def rotate(odd, g, cosine, sine, swap, x, down_t, up):
    rows, width = g.shape
    block = 256
    spec = lambda cols: pl.BlockSpec((block, cols), lambda i, odd: (i, 0))
    whole = lambda a: pl.BlockSpec(a.shape, lambda i, odd: (0, 0))
    return pl.pallas_call(
        rotate_kernel,
        grid_spec=pltpu.PrefetchScalarGridSpec(
            num_scalar_prefetch=1,
            grid=(rows // block,),
            in_specs=[
                spec(width),
                spec(HEAD),
                spec(HEAD),
                whole(swap),
                spec(x.shape[1]),
                whole(down_t),
                whole(up),
            ],
            out_specs=[spec(width), pl.BlockSpec((2 * RANK, block), lambda i, odd: (0, i))],
        ),
        out_shape=[
            jax.ShapeDtypeStruct((rows, width), BF16),
            jax.ShapeDtypeStruct((2 * RANK, rows), F32),
        ],
        compiler_params=pltpu.CompilerParams(
            dimension_semantics=("arbitrary",), vmem_limit_bytes=12 << 20
        ),
        cost_estimate=pl.CostEstimate(
            flops=2 * rows * width * 160, bytes_accessed=8 * rows * width, transcendentals=0
        ),
    )(odd, g, cosine, sine, swap, x, down_t, up)


def product_kernel(adds, s_ref, a_ref, b_ref, *refs):
    pieces, rest = refs[:10], refs[10:]
    out_ref = rest[-1]
    left = jnp.concatenate([a_ref[...], b_ref[...]], axis=1)
    for r in range(4):
        if r == 2:
            kept = jnp.concatenate([pieces[4][0], pieces[5][0]], axis=0)
            other = jnp.concatenate([pieces[6][0], pieces[7][0]], axis=0)
        else:
            at = {0: 0, 1: 2, 3: 8}[r]
            kept, other = pieces[at][0], pieces[at + 1][0]
        total = nt(left, jnp.concatenate([kept, other], axis=1))
        to = s_ref[1 + r]
        if adds:
            total = total + rest[0][to].astype(F32)
        out_ref[to] = total.astype(BF16)


def product(scalars, a, b, pieces, extra=None):
    rows, width = a.shape
    block = 256
    cols = pieces[0].shape[1]
    rows_spec = pl.BlockSpec((block, width), lambda i, s: (i, 0))
    out_spec = pl.BlockSpec((4, block, cols), lambda i, s: (0, i, 0))
    piece_specs = [pl.BlockSpec((1, *p.shape[1:]), lambda i, s: (s[0], 0, 0)) for p in pieces]
    args = [scalars, a, b, *pieces]
    in_specs = [rows_spec, rows_spec, *piece_specs]
    if extra is not None:
        args.append(extra)
        in_specs.append(out_spec)
    return pl.pallas_call(
        functools.partial(product_kernel, extra is not None),
        grid_spec=pltpu.PrefetchScalarGridSpec(
            num_scalar_prefetch=1, grid=(rows // block,), in_specs=in_specs, out_specs=out_spec
        ),
        out_shape=jax.ShapeDtypeStruct((4, rows, cols), BF16),
        compiler_params=pltpu.CompilerParams(
            dimension_semantics=("arbitrary",), vmem_limit_bytes=20 << 20
        ),
        cost_estimate=pl.CostEstimate(
            flops=2 * rows * 2 * width * 4 * cols,
            bytes_accessed=2 * (2 * rows * width + 8 * cols * width + 4 * rows * cols),
            transcendentals=0,
        ),
    )(*args)


def reduce_over_x(parts):
    half = parts.shape[1] // 2
    top, low = parts[:, :half], parts[:, half:]
    far_up = send(top[2], dx=1)
    far_down = send(low[2], dx=-1)
    up_low = send(low[1], dx=1)
    down_top = send(top[3], dx=-1)
    up_top = send((top[1].astype(F32) + far_up.astype(F32)).astype(BF16), dx=1)
    down_low = send((low[3].astype(F32) + far_down.astype(F32)).astype(BF16), dx=-1)
    first = top[0].astype(F32) + up_top.astype(F32) + down_top.astype(F32)
    second = low[0].astype(F32) + up_low.astype(F32) + down_low.astype(F32)
    return jnp.concatenate([first, second], axis=0)


def on_device(normed_input, positions, weight, down, up, gradient):
    rows, width = gradient.shape
    dp, tensor = lax.axis_index("dp"), lax.axis_index("tensor")
    zh, y = dp // 4, dp % 4
    zl, x, k = tensor // 8, (tensor // 2) % 4, tensor % 2

    quarters = weight.reshape(2, 2, weight.shape[0] // 4, width)
    kept = lax.dynamic_index_in_dim(quarters, zl, 1, keepdims=False)
    given = lax.dynamic_index_in_dim(quarters, 1 - zl, 1, keepdims=False)
    other = send(given, zx=1)
    half = kept.shape[1] // 2
    k_prev, k_next = send(kept, dy=1), send(kept, dy=-1)
    o_prev, o_next = send(other, dy=1), send(other, dy=-1)
    k_far = send(k_prev[:, :half], dy=1), send(k_next[:, half:], dy=-1)
    o_far = send(o_prev[:, :half], dy=1), send(o_next[:, half:], dy=-1)
    pieces = (kept, other, k_next, o_next, k_far[0], k_far[1], o_far[0], o_far[1], k_prev, o_prev)

    lanes = jnp.arange(HEAD, dtype=jnp.int32)
    pair = (lanes // 2).astype(F32)
    freq = jnp.float32(500000.0) ** (-2.0 * pair / HEAD)
    angle = positions.astype(F32)[:, None] * freq[None, :]
    row, col = lanes[:, None], lanes[None, :]
    swap = jnp.where(row == (col ^ 1), jnp.where(col % 2 == 0, 1.0, -1.0), 0.0).astype(BF16)
    odd = ((tensor * K_SHARD) % HEAD // K_SHARD).astype(jnp.int32).reshape(1)
    grad_y, low = rotate(
        odd, gradient, jnp.cos(angle), jnp.sin(angle), swap, normed_input, down.T, up
    )

    near = send(grad_y, zx=1)
    cross = send(grad_y, zx=3)
    mid = rows // 2
    far_top = send(cross[:mid], zx=1)
    far_low = send(near[mid:], zx=3)
    far = jnp.concatenate([far_top, far_low], axis=0)

    distance = [(y + r - x) % 4 for r in range(4)]
    theirs = jnp.stack([1 - k, *distance]).astype(jnp.int32)
    mine = jnp.stack([k, *distance]).astype(jnp.int32)
    sums = []
    for a, b in ((grad_y, near), (far, cross)):
        arrived = send(product(theirs, a, b, pieces), dk=1)
        sums.append(reduce_over_x(product(mine, a, b, pieces, arrived)).astype(BF16))
    own, opposite = sums

    low = low + send(low, dk=1)
    low = low + send(low, xx=1)
    low = low + send(low, xx=3)
    low = low + send(low, zx=1)
    low = low.astype(BF16)
    low_x, low_g = low[:RANK], low[RANK:]
    factor = 2.0 / math.sqrt(rows * 8)
    part_a = factor * jnp.dot(low_g, normed_input, preferred_element_type=F32)
    part_b = factor * jnp.dot(low_x, grad_y, preferred_element_type=F32)
    parts = jnp.concatenate([part_a, part_b], axis=1)
    parts = parts + send(parts, yx=1)
    parts = parts + send(parts, yx=3)
    parts = parts + send(parts, zx=2)
    grad_a, grad_b = parts[:, : down.shape[0]].T, parts[:, down.shape[0] :]
    adapter = 2.0 * lax.dot_general(
        low_g, down, (((0,), (1,)), ((), ())), preferred_element_type=F32
    )

    own_moved = send(own, zmap={1: 0, 2: 3})
    far_moved = send(opposite, zmap={0: 2, 3: 1})
    near_moved = send(opposite, zmap={1: 2, 2: 1})
    stays = zh == zl
    first = jnp.where(stays, own, far_moved)
    second = jnp.where(stays, own_moved, near_moved)
    left = jnp.where(zl == 0, first, second)
    right = jnp.where(zl == 0, second, first)
    grad_x = (jnp.concatenate([left, right], axis=1).astype(F32) + adapter).astype(BF16)
    return grad_x, grad_a, grad_b


def solution(mesh):
    placed = (
        P("dp", "tensor"),
        P("dp"),
        P("dp", "tensor"),
        P("tensor", None),
        P(None, "tensor"),
        P("dp", "tensor"),
    )
    return jax.shard_map(
        on_device,
        mesh=mesh,
        in_specs=placed,
        out_specs=(P("dp", "tensor"), P("tensor", None), P(None, "tensor")),
        check_vma=False,
    )
```

```python
import functools
import math

import jax
import jax.numpy as jnp
from jax import lax
from jax.experimental import pallas as pl
from jax.experimental.pallas import tpu as pltpu
from jax.sharding import PartitionSpec as P


HEAD = 128
K_SHARD = 64
RANK = 16
AXES = ("dp", "tensor")
BF16 = jnp.bfloat16
F32 = jnp.float32


def number(x, y, z, k):
    return ((z // 2) * 4 + y) * 16 + (z % 2) * 8 + x * 2 + k


CHIPS = [(x, y, z, k) for x in range(4) for y in range(4) for z in range(4) for k in range(2)]


def send(value, dx=0, dy=0, dk=0, zx=0, xx=0, yx=0, zmap=None):
    pairs = []
    for x, y, z, k in CHIPS:
        if zmap is None:
            to = z ^ zx
        elif z in zmap:
            to = zmap[z]
        else:
            continue
        pairs.append(
            (number(x, y, z, k), number(((x + dx) % 4) ^ xx, ((y + dy) % 4) ^ yx, to, k ^ dk))
        )
    return lax.ppermute(value, AXES, pairs)


def nt(a, b):
    return lax.dot_general(a, b, (((1,), (1,)), ((), ())), preferred_element_type=F32)


def place():
    dp, tensor = lax.axis_index("dp"), lax.axis_index("tensor")
    return dp // 4, dp % 4, tensor // 8, (tensor // 2) % 4, tensor % 2


def rotate_kernel(g_ref, cos_ref, sin_ref, swap_ref, x_ref, down_ref, up_ref, y_ref, low_ref):
    cosine = cos_ref[...]
    sine = sin_ref[...]
    odd = (lax.axis_index("tensor") * K_SHARD) % HEAD == K_SHARD
    lane = lax.broadcasted_iota(jnp.int32, cosine.shape, 1)
    key_cos = jnp.where(odd, pltpu.roll(cosine, 64, 1), cosine)
    key_sin = jnp.where(odd, pltpu.roll(sine, 64, 1), sine)
    key_cos = jnp.where(lane < K_SHARD, key_cos, 1.0)
    key_sin = jnp.where(lane < K_SHARD, key_sin, 0.0)
    groups = g_ref.shape[1] // HEAD
    for i in range(groups):
        g = g_ref[:, i * HEAD : (i + 1) * HEAD]
        turned = jnp.dot(g, swap_ref[...], preferred_element_type=F32)
        c = cosine if i < groups - 1 else key_cos
        s = sine if i < groups - 1 else key_sin
        y_ref[:, i * HEAD : (i + 1) * HEAD] = (g.astype(F32) * c + turned * s).astype(BF16)
    low_ref[:RANK, :] = nt(down_ref[...], x_ref[...])
    low_ref[RANK:, :] = nt(up_ref[...], y_ref[...])


def rotate(g, cosine, sine, swap, x, down_t, up):
    rows, width = g.shape
    block = 256
    spec = lambda cols: pl.BlockSpec((block, cols), lambda i: (i, 0))
    whole = lambda a: pl.BlockSpec(a.shape, lambda i: (0, 0))
    return pl.pallas_call(
        rotate_kernel,
        grid=(rows // block,),
        in_specs=[
            spec(width),
            spec(HEAD),
            spec(HEAD),
            whole(swap),
            spec(x.shape[1]),
            whole(down_t),
            whole(up),
        ],
        out_specs=[spec(width), pl.BlockSpec((2 * RANK, block), lambda i: (0, i))],
        out_shape=[
            jax.ShapeDtypeStruct((rows, width), BF16),
            jax.ShapeDtypeStruct((2 * RANK, rows), F32),
        ],
        compiler_params=pltpu.CompilerParams(
            dimension_semantics=("arbitrary",), vmem_limit_bytes=12 << 20
        ),
        cost_estimate=pl.CostEstimate(
            flops=2 * rows * width * 160, bytes_accessed=8 * rows * width, transcendentals=0
        ),
    )(g, cosine, sine, swap, x, down_t, up)


def product_kernel(chunks, adds, *refs):
    a_refs, b_refs, pieces = refs[:chunks], refs[chunks : 2 * chunks], refs[2 * chunks :]
    out_refs = refs[-2:] if adds else refs[-1:]
    _, y, _, x, k = place()
    core = k if adds else 1 - k
    block = 512
    rows = block * 2
    each = a_refs[0].shape[0] // block
    for i in range(rows // block):
        at = pl.ds((i % each) * block, block)
        left = jnp.concatenate([a_refs[i // each][at, :], b_refs[i // each][at, :]], axis=1)
        for r in range(4):
            if r == 2:
                from_prev, from_next = pieces[4], pieces[5]
                kept = jnp.concatenate([from_prev[0, core], from_next[0, core]], axis=0)
                other = jnp.concatenate([from_prev[1, core], from_next[1, core]], axis=0)
            else:
                first = {0: 0, 1: 2, 3: 6}[r]
                kept, other = pieces[first][core], pieces[first + 1][core]
            total = nt(left, jnp.concatenate([kept, other], axis=1))
            to = (y + r + 4 - x) % 4
            if adds:
                total = total + refs[-3][to, i * block : (i + 1) * block, :].astype(F32)
                out_refs[i][to] = total.astype(BF16)
            else:
                out_refs[0][to, i * block : (i + 1) * block, :] = total.astype(BF16)


def product(a, b, pieces, extra=None):
    rows = sum(c.shape[0] for c in a)
    width = a[0].shape[1]
    cols = pieces[0].shape[1]
    args = [*a, *b, *pieces]
    if extra is not None:
        args.append(extra)
    vmem = pl.BlockSpec(memory_space=pltpu.VMEM)
    return pl.pallas_call(
        functools.partial(product_kernel, len(a), extra is not None),
        in_specs=[vmem] * len(args),
        out_specs=vmem if extra is None else [vmem] * 2,
        out_shape=jax.ShapeDtypeStruct((4, rows, cols), BF16)
        if extra is None
        else [jax.ShapeDtypeStruct((4, rows // 2, cols), BF16)] * 2,
        compiler_params=pltpu.CompilerParams(vmem_limit_bytes=16 << 20),
        cost_estimate=pl.CostEstimate(
            flops=2 * rows * 2 * width * 4 * cols,
            bytes_accessed=2 * (2 * rows * width + 8 * cols * width + 4 * rows * cols),
            transcendentals=0,
        ),
    )(*args)


def adapters_kernel(factor, low_ref, more_ref, x_ref, y_ref, low_out, parts_ref):
    low = (low_ref[...] + more_ref[...]).astype(BF16)
    low_out[...] = low
    depth = x_ref.shape[1]
    parts_ref[:, :depth] = factor * jnp.dot(low[RANK:], x_ref[...], preferred_element_type=F32)
    parts_ref[:, depth:] = factor * jnp.dot(low[:RANK], y_ref[...], preferred_element_type=F32)


def adapters(factor, low, more, x, grad_y):
    vmem = pl.BlockSpec(memory_space=pltpu.VMEM)
    cols = x.shape[1] + grad_y.shape[1]
    return pl.pallas_call(
        functools.partial(adapters_kernel, factor),
        in_specs=[vmem] * 4,
        out_specs=[vmem] * 2,
        out_shape=[
            jax.ShapeDtypeStruct(low.shape, BF16),
            jax.ShapeDtypeStruct((RANK, cols), F32),
        ],
        compiler_params=pltpu.CompilerParams(vmem_limit_bytes=12 << 20),
        cost_estimate=pl.CostEstimate(
            flops=16 * RANK * x.shape[0] * cols, bytes_accessed=2 * x.shape[0] * cols, transcendentals=0
        ),
    )(low, more, x, grad_y)


def finish_kernel(own_ref, own_moved_ref, far_moved_ref, near_moved_ref, low_ref, down_ref, out_ref):
    zh, _, zl, _, _ = place()
    stays = zh == zl
    first = jnp.where(stays, own_ref[...], far_moved_ref[...])
    second = jnp.where(stays, own_moved_ref[...], near_moved_ref[...])
    adapter = 2.0 * lax.dot_general(
        low_ref[RANK:], down_ref[...], (((0,), (0,)), ((), ())), preferred_element_type=F32
    )
    cols = own_ref.shape[1]
    left = jnp.where(zl == 0, first, second)
    right = jnp.where(zl == 0, second, first)
    out_ref[:, :cols] = (left.astype(F32) + adapter[:, :cols]).astype(BF16)
    out_ref[:, cols:] = (right.astype(F32) + adapter[:, cols:]).astype(BF16)


def finish(own, own_moved, far_moved, near_moved, low, down_t):
    rows, cols = own.shape
    block = 256
    half = pl.BlockSpec((block, cols), lambda i: (i, 0))
    return pl.pallas_call(
        finish_kernel,
        grid=(rows // block,),
        in_specs=[half] * 4
        + [
            pl.BlockSpec((2 * RANK, block), lambda i: (0, i)),
            pl.BlockSpec(down_t.shape, lambda i: (0, 0)),
        ],
        out_specs=pl.BlockSpec((block, 2 * cols), lambda i: (i, 0)),
        out_shape=jax.ShapeDtypeStruct((rows, 2 * cols), BF16),
        compiler_params=pltpu.CompilerParams(
            dimension_semantics=("arbitrary",), vmem_limit_bytes=8 << 20
        ),
        cost_estimate=pl.CostEstimate(
            flops=64 * rows * cols, bytes_accessed=12 * rows * cols, transcendentals=0
        ),
    )(own, own_moved, far_moved, near_moved, low, down_t)


def reduce_over_x(top, low):
    far_up = send(top[2], dx=1)
    far_down = send(low[2], dx=-1)
    up_low = send(low[1], dx=1)
    down_top = send(top[3], dx=-1)
    up_top = send((top[1].astype(F32) + far_up.astype(F32)).astype(BF16), dx=1)
    down_low = send((low[3].astype(F32) + far_down.astype(F32)).astype(BF16), dx=-1)
    first = top[0].astype(F32) + up_top.astype(F32) + down_top.astype(F32)
    second = low[0].astype(F32) + up_low.astype(F32) + down_low.astype(F32)
    return jnp.concatenate([first, second], axis=0)


def in_order(normed_input, positions, weight, down, up, gradient):
    rows, width = gradient.shape
    zl = lax.axis_index("tensor") // 8

    quarters = weight.reshape(2, 2, weight.shape[0] // 4, width)
    kept = lax.dynamic_index_in_dim(quarters, zl, 1, keepdims=False)
    given = lax.dynamic_index_in_dim(quarters, 1 - zl, 1, keepdims=False)
    other = send(given, zx=1)
    half = kept.shape[1] // 2
    k_prev, k_next = send(kept, dy=1), send(kept, dy=-1)
    o_prev, o_next = send(other, dy=1), send(other, dy=-1)
    far_prev = send(jnp.stack([k_prev[:, :half], o_prev[:, :half]]), dy=1)
    far_next = send(jnp.stack([k_next[:, half:], o_next[:, half:]]), dy=-1)
    pieces = (kept, other, k_next, o_next, far_prev, far_next, k_prev, o_prev)

    lanes = jnp.arange(HEAD, dtype=jnp.int32)
    pair = (lanes // 2).astype(F32)
    freq = jnp.float32(500000.0) ** (-2.0 * pair / HEAD)
    angle = positions.astype(F32)[:, None] * freq[None, :]
    row, col = lanes[:, None], lanes[None, :]
    swap = jnp.where(row == (col ^ 1), jnp.where(col % 2 == 0, 1.0, -1.0), 0.0).astype(BF16)
    cosine, sine, down_t = jnp.cos(angle), jnp.sin(angle), down.T
    grad_y, low = rotate(gradient, cosine, sine, swap, normed_input, down_t, up)

    near = send(grad_y, zx=1)
    cross = send(grad_y, zx=3)
    mid = rows // 2
    far_top = send(cross[:mid], zx=1)
    far_low = send(near[mid:], zx=3)

    low = low + send(low, zx=1)
    low = low + send(low, dk=1)
    low = low + send(low, xx=1)
    more = send(low, xx=3)
    factor = 2.0 / math.sqrt(rows * 8)
    low, parts = adapters(factor, low, more, normed_input, grad_y)
    parts = parts + send(parts, yx=1)
    parts = parts + send(parts, yx=3)
    parts = parts + send(parts, zx=2)
    grad_a, grad_b = parts[:, : down.shape[0]].T, parts[:, down.shape[0] :]

    sums = []
    for a, b in (([grad_y], [near]), ([far_top, far_low], [cross])):
        if len(a) != len(b):
            b = [b[0][:mid], b[0][mid:]]
        partial = product(a, b, pieces)
        arrived = send(partial, dk=1)
        top, low_half = product(a, b, pieces, arrived)
        sums.append(reduce_over_x(top, low_half).astype(BF16))
    own, opposite = sums

    own_moved = send(own, zmap={1: 0, 2: 3})
    far_moved = send(opposite, zmap={0: 2, 3: 1})
    near_moved = send(opposite, zmap={1: 2, 2: 1})
    grad_x = finish(own, own_moved, far_moved, near_moved, low, down_t)
    return grad_x, grad_a, grad_b


def solution(mesh):
    placed = (
        P("dp", "tensor"),
        P("dp"),
        P("dp", "tensor"),
        P("tensor", None),
        P(None, "tensor"),
        P("dp", "tensor"),
    )
    return jax.shard_map(
        in_order,
        mesh=mesh,
        in_specs=placed,
        out_specs=(P("dp", "tensor"), P("tensor", None), P(None, "tensor")),
        check_vma=False,
    )
```

```python
import functools
import math

import jax
import jax.numpy as jnp
from jax import lax
from jax.experimental import pallas as pl
from jax.experimental.pallas import tpu as pltpu
from jax.sharding import PartitionSpec as P


HEAD = 128
K_SHARD = 64
RANK = 16
AXES = ("dp", "tensor")
BF16 = jnp.bfloat16
F32 = jnp.float32


def number(x, y, z, k):
    return ((z // 2) * 4 + y) * 16 + (z % 2) * 8 + x * 2 + k


CHIPS = [(x, y, z, k) for x in range(4) for y in range(4) for z in range(4) for k in range(2)]


def send(value, dx=0, dy=0, dk=0, zx=0, xx=0, yx=0, zmap=None):
    pairs = []
    for x, y, z, k in CHIPS:
        if zmap is None:
            to = z ^ zx
        elif z in zmap:
            to = zmap[z]
        else:
            continue
        pairs.append(
            (number(x, y, z, k), number(((x + dx) % 4) ^ xx, ((y + dy) % 4) ^ yx, to, k ^ dk))
        )
    return lax.ppermute(value, AXES, pairs)


def nt(a, b):
    return lax.dot_general(a, b, (((1,), (1,)), ((), ())), preferred_element_type=F32)


def place():
    dp, tensor = lax.axis_index("dp"), lax.axis_index("tensor")
    return dp // 4, dp % 4, tensor // 8, (tensor // 2) % 4, tensor % 2


def rotate_kernel(g_ref, cos_ref, sin_ref, swap_ref, x_ref, down_ref, up_ref, y_ref, low_ref):
    cosine = cos_ref[...]
    sine = sin_ref[...]
    odd = (lax.axis_index("tensor") * K_SHARD) % HEAD == K_SHARD
    lane = lax.broadcasted_iota(jnp.int32, cosine.shape, 1)
    key_cos = jnp.where(odd, pltpu.roll(cosine, 64, 1), cosine)
    key_sin = jnp.where(odd, pltpu.roll(sine, 64, 1), sine)
    key_cos = jnp.where(lane < K_SHARD, key_cos, 1.0)
    key_sin = jnp.where(lane < K_SHARD, key_sin, 0.0)
    groups = g_ref.shape[1] // HEAD
    for i in range(groups):
        g = g_ref[:, i * HEAD : (i + 1) * HEAD]
        turned = jnp.dot(g, swap_ref[...], preferred_element_type=F32)
        c = cosine if i < groups - 1 else key_cos
        s = sine if i < groups - 1 else key_sin
        y_ref[:, i * HEAD : (i + 1) * HEAD] = (g.astype(F32) * c + turned * s).astype(BF16)
    low_ref[:RANK, :] = nt(down_ref[...], x_ref[...])
    low_ref[RANK:, :] = nt(up_ref[...], y_ref[...])


def rotate(g, cosine, sine, swap, x, down_t, up):
    rows, width = g.shape
    block = 256
    spec = lambda cols: pl.BlockSpec((block, cols), lambda i: (i, 0))
    whole = lambda a: pl.BlockSpec(a.shape, lambda i: (0, 0))
    return pl.pallas_call(
        rotate_kernel,
        grid=(rows // block,),
        in_specs=[
            spec(width),
            spec(HEAD),
            spec(HEAD),
            whole(swap),
            spec(x.shape[1]),
            whole(down_t),
            whole(up),
        ],
        out_specs=[spec(width), pl.BlockSpec((2 * RANK, block), lambda i: (0, i))],
        out_shape=[
            jax.ShapeDtypeStruct((rows, width), BF16),
            jax.ShapeDtypeStruct((2 * RANK, rows), F32),
        ],
        compiler_params=pltpu.CompilerParams(
            dimension_semantics=("arbitrary",), vmem_limit_bytes=12 << 20
        ),
        cost_estimate=pl.CostEstimate(
            flops=2 * rows * width * 160, bytes_accessed=8 * rows * width, transcendentals=0
        ),
    )(g, cosine, sine, swap, x, down_t, up)


def product_kernel(chunks, keep, *refs):
    a_refs, b_refs, pieces = refs[:chunks], refs[chunks : 2 * chunks], refs[2 * chunks :]
    out_refs = refs[-2:]
    _, y, _, x, k = place()
    core = k if keep else 1 - k
    block = out_refs[0].shape[1]
    each = a_refs[0].shape[0] // block
    for i in range(2):
        at = pl.ds((i % each) * block, block)
        left = jnp.concatenate([a_refs[i // each][at, :], b_refs[i // each][at, :]], axis=1)
        for r in range(4):
            if r == 2:
                kept = jnp.concatenate([pieces[4][core], pieces[5][core]], axis=0)
                other = jnp.concatenate([pieces[6][core], pieces[7][core]], axis=0)
            else:
                first = {0: 0, 1: 2, 3: 8}[r]
                kept, other = pieces[first][core], pieces[first + 1][core]
            total = nt(left, jnp.concatenate([kept, other], axis=1))
            to = (y + r + 4 - x) % 4
            out_refs[i][to] = total.astype(out_refs[i].dtype)


def product(a, b, pieces, keep):
    rows = sum(c.shape[0] for c in a)
    width = a[0].shape[1]
    cols = pieces[0].shape[1]
    args = [*a, *b, *pieces]
    vmem = pl.BlockSpec(memory_space=pltpu.VMEM)
    return pl.pallas_call(
        functools.partial(product_kernel, len(a), keep),
        in_specs=[vmem] * len(args),
        out_specs=[vmem] * 2,
        out_shape=[jax.ShapeDtypeStruct((4, rows // 2, cols), F32 if keep else BF16)] * 2,
        compiler_params=pltpu.CompilerParams(vmem_limit_bytes=16 << 20),
        cost_estimate=pl.CostEstimate(
            flops=2 * rows * 2 * width * 4 * cols,
            bytes_accessed=2 * (2 * rows * width + 8 * cols * width + 4 * rows * cols),
            transcendentals=0,
        ),
    )(*args)


def adapters_kernel(factor, low_ref, more_ref, x_ref, y_ref, low_out, parts_ref):
    low = (low_ref[...] + more_ref[...]).astype(BF16)
    low_out[...] = low
    depth = x_ref.shape[1]
    parts_ref[:, :depth] = factor * jnp.dot(low[RANK:], x_ref[...], preferred_element_type=F32)
    parts_ref[:, depth:] = factor * jnp.dot(low[:RANK], y_ref[...], preferred_element_type=F32)


def adapters(factor, low, more, x, grad_y):
    vmem = pl.BlockSpec(memory_space=pltpu.VMEM)
    cols = x.shape[1] + grad_y.shape[1]
    return pl.pallas_call(
        functools.partial(adapters_kernel, factor),
        in_specs=[vmem] * 4,
        out_specs=[vmem] * 2,
        out_shape=[
            jax.ShapeDtypeStruct(low.shape, BF16),
            jax.ShapeDtypeStruct((RANK, cols), F32),
        ],
        compiler_params=pltpu.CompilerParams(vmem_limit_bytes=12 << 20),
        cost_estimate=pl.CostEstimate(
            flops=16 * RANK * x.shape[0] * cols, bytes_accessed=2 * x.shape[0] * cols, transcendentals=0
        ),
    )(low, more, x, grad_y)


def finish_kernel(own_ref, own_moved_ref, far_moved_ref, near_moved_ref, low_ref, down_ref, out_ref):
    zh, _, zl, _, _ = place()
    stays = zh == zl
    first = jnp.where(stays, own_ref[...], far_moved_ref[...])
    second = jnp.where(stays, own_moved_ref[...], near_moved_ref[...])
    adapter = 2.0 * lax.dot_general(
        low_ref[RANK:], down_ref[...], (((0,), (0,)), ((), ())), preferred_element_type=F32
    )
    cols = own_ref.shape[1]
    left = jnp.where(zl == 0, first, second)
    right = jnp.where(zl == 0, second, first)
    out_ref[:, :cols] = (left.astype(F32) + adapter[:, :cols]).astype(BF16)
    out_ref[:, cols:] = (right.astype(F32) + adapter[:, cols:]).astype(BF16)


def finish(own, own_moved, far_moved, near_moved, low, down_t):
    rows, cols = own.shape
    block = 256
    half = pl.BlockSpec((block, cols), lambda i: (i, 0))
    return pl.pallas_call(
        finish_kernel,
        grid=(rows // block,),
        in_specs=[half] * 4
        + [
            pl.BlockSpec((2 * RANK, block), lambda i: (0, i)),
            pl.BlockSpec(down_t.shape, lambda i: (0, 0)),
        ],
        out_specs=pl.BlockSpec((block, 2 * cols), lambda i: (i, 0)),
        out_shape=jax.ShapeDtypeStruct((rows, 2 * cols), BF16),
        compiler_params=pltpu.CompilerParams(
            dimension_semantics=("arbitrary",), vmem_limit_bytes=8 << 20
        ),
        cost_estimate=pl.CostEstimate(
            flops=64 * rows * cols, bytes_accessed=12 * rows * cols, transcendentals=0
        ),
    )(own, own_moved, far_moved, near_moved, low, down_t)


def add_up_kernel(*refs):
    kept, arrived, ups, downs, out_ref = refs[:2], refs[2:4], refs[4:6], refs[6:8], refs[8]
    rows = ups[0].shape[0]
    for i in range(2):
        total = kept[i][0] + arrived[i][0].astype(F32)
        total = total + ups[i][...].astype(F32) + downs[i][...].astype(F32)
        out_ref[i * rows : (i + 1) * rows, :] = total.astype(BF16)


def add_up(kept, arrived, ups, downs):
    rows, cols = ups[0].shape
    vmem = pl.BlockSpec(memory_space=pltpu.VMEM)
    return pl.pallas_call(
        add_up_kernel,
        in_specs=[vmem] * 8,
        out_specs=vmem,
        out_shape=jax.ShapeDtypeStruct((2 * rows, cols), BF16),
        compiler_params=pltpu.CompilerParams(vmem_limit_bytes=14 << 20),
        cost_estimate=pl.CostEstimate(
            flops=8 * rows * cols, bytes_accessed=24 * rows * cols, transcendentals=0
        ),
    )(*kept, *arrived, *ups, *downs)


def reduce_over_x(kept, arrived):
    def term(to, low):
        return kept[low][to] + arrived[low][to].astype(F32)

    far_up = send(term(2, False).astype(BF16), dx=1)
    far_down = send(term(2, True).astype(BF16), dx=-1)
    up_low = send(term(1, True).astype(BF16), dx=1)
    down_top = send(term(3, False).astype(BF16), dx=-1)
    up_top = send((term(1, False) + far_up.astype(F32)).astype(BF16), dx=1)
    down_low = send((term(3, True) + far_down.astype(F32)).astype(BF16), dx=-1)
    return add_up(kept, arrived, (up_top, up_low), (down_top, down_low))


def in_order(normed_input, positions, weight, down, up, gradient):
    rows, width = gradient.shape
    zl = lax.axis_index("tensor") // 8

    quarters = weight.reshape(2, 2, weight.shape[0] // 4, width)
    kept = lax.dynamic_index_in_dim(quarters, zl, 1, keepdims=False)
    given = lax.dynamic_index_in_dim(quarters, 1 - zl, 1, keepdims=False)
    other = send(given, zx=1)
    half = kept.shape[1] // 2
    k_prev, k_next = send(kept, dy=1), send(kept, dy=-1)
    o_prev, o_next = send(other, dy=1), send(other, dy=-1)
    k_far = send(k_prev[:, :half], dy=1), send(k_next[:, half:], dy=-1)
    o_far = send(o_prev[:, :half], dy=1), send(o_next[:, half:], dy=-1)
    pieces = (kept, other, k_next, o_next, *k_far, *o_far, k_prev, o_prev)

    lanes = jnp.arange(HEAD, dtype=jnp.int32)
    pair = (lanes // 2).astype(F32)
    freq = jnp.float32(500000.0) ** (-2.0 * pair / HEAD)
    angle = positions.astype(F32)[:, None] * freq[None, :]
    row, col = lanes[:, None], lanes[None, :]
    swap = jnp.where(row == (col ^ 1), jnp.where(col % 2 == 0, 1.0, -1.0), 0.0).astype(BF16)
    cosine, sine, down_t = jnp.cos(angle), jnp.sin(angle), down.T
    grad_y, low = rotate(gradient, cosine, sine, swap, normed_input, down_t, up)

    near = send(grad_y, zx=1)
    cross = send(grad_y, zx=3)
    mid = rows // 2
    far_top = send(cross[:mid], zx=1)
    far_low = send(near[mid:], zx=3)

    low = low + send(low, zx=1)
    low = low + send(low, dk=1)
    low = low + send(low, xx=1)
    more = send(low, xx=3)
    factor = 2.0 / math.sqrt(rows * 8)
    low, parts = adapters(factor, low, more, normed_input, grad_y)
    parts = parts + send(parts, yx=1)
    parts = parts + send(parts, yx=3)
    parts = parts + send(parts, zx=2)
    grad_a, grad_b = parts[:, : down.shape[0]].T, parts[:, down.shape[0] :]

    sums = []
    for a, b in (([grad_y], [near]), ([far_top, far_low], [cross])):
        if len(a) != len(b):
            b = [b[0][:mid], b[0][mid:]]
        partial = product(a, b, pieces, False)
        arrived = [send(p, dk=1) for p in partial]
        total = product(a, b, pieces, True)
        sums.append(reduce_over_x(total, arrived))
    own, opposite = sums

    own_moved = send(own, zmap={1: 0, 2: 3})
    far_moved = send(opposite, zmap={0: 2, 3: 1})
    near_moved = send(opposite, zmap={1: 2, 2: 1})
    grad_x = finish(own, own_moved, far_moved, near_moved, low, down_t)
    return grad_x, grad_a, grad_b


def solution(mesh):
    placed = (
        P("dp", "tensor"),
        P("dp"),
        P("dp", "tensor"),
        P("tensor", None),
        P(None, "tensor"),
        P("dp", "tensor"),
    )
    return jax.shard_map(
        in_order,
        mesh=mesh,
        in_specs=placed,
        out_specs=(P("dp", "tensor"), P("tensor", None), P(None, "tensor")),
        check_vma=False,
    )
```

```python
import functools
import math

import jax
import jax.numpy as jnp
from jax import lax
from jax.experimental import pallas as pl
from jax.experimental.pallas import tpu as pltpu
from jax.sharding import PartitionSpec as P


HEAD = 128
K_SHARD = 64
RANK = 16
AXES = ("dp", "tensor")
BF16 = jnp.bfloat16
F32 = jnp.float32


def number(x, y, z, k):
    return ((z // 2) * 4 + y) * 16 + (z % 2) * 8 + x * 2 + k


CHIPS = [(x, y, z, k) for x in range(4) for y in range(4) for z in range(4) for k in range(2)]


def send(value, dx=0, dy=0, dk=0, zx=0, xx=0, yx=0, zmap=None):
    pairs = []
    for x, y, z, k in CHIPS:
        if zmap is None:
            to = z ^ zx
        elif z in zmap:
            to = zmap[z]
        else:
            continue
        pairs.append(
            (number(x, y, z, k), number(((x + dx) % 4) ^ xx, ((y + dy) % 4) ^ yx, to, k ^ dk))
        )
    return lax.ppermute(value, AXES, pairs)


def nt(a, b):
    return lax.dot_general(a, b, (((1,), (1,)), ((), ())), preferred_element_type=F32)


def place():
    dp, tensor = lax.axis_index("dp"), lax.axis_index("tensor")
    return dp // 4, dp % 4, tensor // 8, (tensor // 2) % 4, tensor % 2


def rotate_kernel(g_ref, cos_ref, sin_ref, swap_ref, x_ref, down_ref, up_ref, y_ref, low_ref):
    cosine = cos_ref[...]
    sine = sin_ref[...]
    odd = (lax.axis_index("tensor") * K_SHARD) % HEAD == K_SHARD
    lane = lax.broadcasted_iota(jnp.int32, cosine.shape, 1)
    key_cos = jnp.where(odd, pltpu.roll(cosine, 64, 1), cosine)
    key_sin = jnp.where(odd, pltpu.roll(sine, 64, 1), sine)
    key_cos = jnp.where(lane < K_SHARD, key_cos, 1.0)
    key_sin = jnp.where(lane < K_SHARD, key_sin, 0.0)
    groups = g_ref.shape[1] // HEAD
    for i in range(groups):
        g = g_ref[:, i * HEAD : (i + 1) * HEAD]
        turned = jnp.dot(g, swap_ref[...], preferred_element_type=F32)
        c = cosine if i < groups - 1 else key_cos
        s = sine if i < groups - 1 else key_sin
        y_ref[:, i * HEAD : (i + 1) * HEAD] = (g.astype(F32) * c + turned * s).astype(BF16)
    low_ref[:RANK, :] = nt(down_ref[...], x_ref[...])
    low_ref[RANK:, :] = nt(up_ref[...], y_ref[...])


def rotate(g, cosine, sine, swap, x, down_t, up):
    rows, width = g.shape
    block = 256
    spec = lambda cols: pl.BlockSpec((block, cols), lambda i: (i, 0))
    whole = lambda a: pl.BlockSpec(a.shape, lambda i: (0, 0))
    return pl.pallas_call(
        rotate_kernel,
        grid=(rows // block,),
        in_specs=[
            spec(width),
            spec(HEAD),
            spec(HEAD),
            whole(swap),
            spec(x.shape[1]),
            whole(down_t),
            whole(up),
        ],
        out_specs=[spec(width), pl.BlockSpec((2 * RANK, block), lambda i: (0, i))],
        out_shape=[
            jax.ShapeDtypeStruct((rows, width), BF16),
            jax.ShapeDtypeStruct((2 * RANK, rows), F32),
        ],
        compiler_params=pltpu.CompilerParams(
            dimension_semantics=("arbitrary",), vmem_limit_bytes=12 << 20
        ),
        cost_estimate=pl.CostEstimate(
            flops=2 * rows * width * 160, bytes_accessed=8 * rows * width, transcendentals=0
        ),
    )(g, cosine, sine, swap, x, down_t, up)


def product_kernel(chunks, keep, *refs):
    a_refs, b_refs, pieces = refs[: chunks[0]], refs[chunks[0] : sum(chunks)], refs[sum(chunks) :]
    out_refs = refs[-2:]
    _, y, _, x, k = place()
    core = k if keep else 1 - k
    block = out_refs[0].shape[1]

    def half(of, i):
        return of[i][...] if len(of) == 2 else of[0][i * block : (i + 1) * block, :]

    for i in range(2):
        left = jnp.concatenate([half(a_refs, i), half(b_refs, i)], axis=1)
        for r in range(4):
            if r == 2:
                kept = jnp.concatenate([pieces[4][core], pieces[5][core]], axis=0)
                other = jnp.concatenate([pieces[6][core], pieces[7][core]], axis=0)
            else:
                first = {0: 0, 1: 2, 3: 8}[r]
                kept, other = pieces[first][core], pieces[first + 1][core]
            total = nt(left, jnp.concatenate([kept, other], axis=1))
            to = (y + r + 4 - x) % 4
            out_refs[i][to] = total.astype(out_refs[i].dtype)


def product(a, b, pieces, keep):
    rows = sum(c.shape[0] for c in a)
    width = a[0].shape[1]
    cols = pieces[0].shape[1]
    args = [*a, *b, *pieces]
    vmem = pl.BlockSpec(memory_space=pltpu.VMEM)
    return pl.pallas_call(
        functools.partial(product_kernel, (len(a), len(b)), keep),
        in_specs=[vmem] * len(args),
        out_specs=[vmem] * 2,
        out_shape=[jax.ShapeDtypeStruct((4, rows // 2, cols), F32 if keep else BF16)] * 2,
        compiler_params=pltpu.CompilerParams(vmem_limit_bytes=16 << 20),
        cost_estimate=pl.CostEstimate(
            flops=2 * rows * 2 * width * 4 * cols,
            bytes_accessed=2 * (2 * rows * width + 8 * cols * width + 4 * rows * cols),
            transcendentals=0,
        ),
    )(*args)


def adapters_kernel(factor, low_ref, more_ref, x_ref, y_ref, low_out, parts_ref):
    low = (low_ref[...] + more_ref[...]).astype(BF16)
    low_out[...] = low
    depth = x_ref.shape[1]
    parts_ref[:, :depth] = factor * jnp.dot(low[RANK:], x_ref[...], preferred_element_type=F32)
    parts_ref[:, depth:] = factor * jnp.dot(low[:RANK], y_ref[...], preferred_element_type=F32)


def adapters(factor, low, more, x, grad_y):
    vmem = pl.BlockSpec(memory_space=pltpu.VMEM)
    cols = x.shape[1] + grad_y.shape[1]
    return pl.pallas_call(
        functools.partial(adapters_kernel, factor),
        in_specs=[vmem] * 4,
        out_specs=[vmem] * 2,
        out_shape=[
            jax.ShapeDtypeStruct(low.shape, BF16),
            jax.ShapeDtypeStruct((RANK, cols), F32),
        ],
        compiler_params=pltpu.CompilerParams(vmem_limit_bytes=12 << 20),
        cost_estimate=pl.CostEstimate(
            flops=16 * RANK * x.shape[0] * cols, bytes_accessed=2 * x.shape[0] * cols, transcendentals=0
        ),
    )(low, more, x, grad_y)


def finish_kernel(
    own_ref, own_moved_ref, far_a, far_b, near_a, near_b, low_ref, down_ref, out_ref
):
    zh, _, zl, _, _ = place()
    stays = zh == zl
    cut = far_a.shape[0]
    cols = own_ref.shape[1]
    block = 128
    for start in range(0, own_ref.shape[0], block):
        at = slice(start, start + block)
        far, near = (far_a[at, :], near_a[at, :]) if start < cut else (
            far_b[start - cut : start - cut + block, :],
            near_b[start - cut : start - cut + block, :],
        )
        first = jnp.where(stays, own_ref[at, :], far)
        second = jnp.where(stays, own_moved_ref[at, :], near)
        adapter = 2.0 * lax.dot_general(
            low_ref[RANK:, at], down_ref[...], (((0,), (0,)), ((), ())), preferred_element_type=F32
        )
        left = jnp.where(zl == 0, first, second)
        right = jnp.where(zl == 0, second, first)
        out_ref[at, :cols] = (left.astype(F32) + adapter[:, :cols]).astype(BF16)
        out_ref[at, cols:] = (right.astype(F32) + adapter[:, cols:]).astype(BF16)


def finish(own, own_moved, far, near, low, down_t):
    rows, cols = own.shape
    vmem = pl.BlockSpec(memory_space=pltpu.VMEM)
    return pl.pallas_call(
        finish_kernel,
        in_specs=[vmem] * 8,
        out_specs=vmem,
        out_shape=jax.ShapeDtypeStruct((rows, 2 * cols), BF16),
        compiler_params=pltpu.CompilerParams(vmem_limit_bytes=12 << 20),
        cost_estimate=pl.CostEstimate(
            flops=64 * rows * cols, bytes_accessed=12 * rows * cols, transcendentals=0
        ),
    )(own, own_moved, *far, *near, low, down_t)


def add_up_kernel(*refs):
    kept, arrived, ups, downs, out_ref = refs[:2], refs[2:4], refs[4:6], refs[6:8], refs[8]
    rows = ups[0].shape[0]
    for i in range(2):
        total = kept[i][0] + arrived[i][0].astype(F32)
        total = total + ups[i][...].astype(F32) + downs[i][...].astype(F32)
        out_ref[i * rows : (i + 1) * rows, :] = total.astype(BF16)


def add_up(kept, arrived, ups, downs):
    rows, cols = ups[0].shape
    vmem = pl.BlockSpec(memory_space=pltpu.VMEM)
    return pl.pallas_call(
        add_up_kernel,
        in_specs=[vmem] * 8,
        out_specs=vmem,
        out_shape=jax.ShapeDtypeStruct((2 * rows, cols), BF16),
        compiler_params=pltpu.CompilerParams(vmem_limit_bytes=14 << 20),
        cost_estimate=pl.CostEstimate(
            flops=8 * rows * cols, bytes_accessed=24 * rows * cols, transcendentals=0
        ),
    )(*kept, *arrived, *ups, *downs)


def reduce_over_x(kept, arrived):
    def term(to, low):
        return kept[low][to] + arrived[low][to].astype(F32)

    far_up = send(term(2, False).astype(BF16), dx=1)
    far_down = send(term(2, True).astype(BF16), dx=-1)
    up_low = send(term(1, True).astype(BF16), dx=1)
    down_top = send(term(3, False).astype(BF16), dx=-1)
    up_top = send((term(1, False) + far_up.astype(F32)).astype(BF16), dx=1)
    down_low = send((term(3, True) + far_down.astype(F32)).astype(BF16), dx=-1)
    return add_up(kept, arrived, (up_top, up_low), (down_top, down_low))


def in_order(normed_input, positions, weight, down, up, gradient):
    rows, width = gradient.shape
    zl = lax.axis_index("tensor") // 8

    quarters = weight.reshape(2, 2, weight.shape[0] // 4, width)
    kept = lax.dynamic_index_in_dim(quarters, zl, 1, keepdims=False)
    given = lax.dynamic_index_in_dim(quarters, 1 - zl, 1, keepdims=False)
    other = send(given, zx=1)
    half = kept.shape[1] // 2
    k_prev, k_next = send(kept, dy=1), send(kept, dy=-1)
    o_prev, o_next = send(other, dy=1), send(other, dy=-1)
    k_far = send(k_prev[:, :half], dy=1), send(k_next[:, half:], dy=-1)
    o_far = send(o_prev[:, :half], dy=1), send(o_next[:, half:], dy=-1)
    pieces = (kept, other, k_next, o_next, *k_far, *o_far, k_prev, o_prev)

    lanes = jnp.arange(HEAD, dtype=jnp.int32)
    pair = (lanes // 2).astype(F32)
    freq = jnp.float32(500000.0) ** (-2.0 * pair / HEAD)
    angle = positions.astype(F32)[:, None] * freq[None, :]
    row, col = lanes[:, None], lanes[None, :]
    swap = jnp.where(row == (col ^ 1), jnp.where(col % 2 == 0, 1.0, -1.0), 0.0).astype(BF16)
    cosine, sine, down_t = jnp.cos(angle), jnp.sin(angle), down.T
    grad_y, low = rotate(gradient, cosine, sine, swap, normed_input, down_t, up)

    mid = rows // 2
    near_low = send(grad_y[mid:], zx=1)
    near_top = send(grad_y[:mid], zx=1)
    cross = send(grad_y, zx=3)
    far_top = send(cross[:mid], zx=1)
    far_low = send(near_low, zx=3)

    low = low + send(low, zx=1)
    low = low + send(low, dk=1)
    low = low + send(low, xx=1)
    more = send(low, xx=3)
    factor = 2.0 / math.sqrt(rows * 8)
    low, parts = adapters(factor, low, more, normed_input, grad_y)
    parts = parts + send(parts, yx=1)
    parts = parts + send(parts, yx=3)
    parts = parts + send(parts, zx=2)
    grad_a, grad_b = parts[:, : down.shape[0]].T, parts[:, down.shape[0] :]

    sums = []
    for a, b in (([grad_y], [near_top, near_low]), ([far_top, far_low], [cross])):
        partial = product(a, b, pieces, False)
        arrived = [send(p, dk=1) for p in partial]
        total = product(a, b, pieces, True)
        sums.append(reduce_over_x(total, arrived))
    own, opposite = sums

    own_moved = send(own, zmap={1: 0, 2: 3})
    cut = 640
    top, low_rows = opposite[:cut], opposite[cut:]
    near_a = send(top, zx=3)
    near_b = send(low_rows, zmap={1: 2, 2: 1})
    far_a = send(near_a, zmap={3: 2, 0: 1})
    far_b = send(low_rows, zmap={0: 2, 3: 1})
    grad_x = finish(own, own_moved, (far_a, far_b), (near_a, near_b), low, down_t)
    return grad_x, grad_a, grad_b


def solution(mesh):
    placed = (
        P("dp", "tensor"),
        P("dp"),
        P("dp", "tensor"),
        P("tensor", None),
        P(None, "tensor"),
        P("dp", "tensor"),
    )
    return jax.shard_map(
        in_order,
        mesh=mesh,
        in_specs=placed,
        out_specs=(P("dp", "tensor"), P("tensor", None), P(None, "tensor")),
        check_vma=False,
    )
```

```python
import functools
import math

import jax
import jax.numpy as jnp
from jax import lax
from jax.experimental import pallas as pl
from jax.experimental.pallas import tpu as pltpu
from jax.sharding import PartitionSpec as P


HEAD = 128
K_SHARD = 64
RANK = 16
AXES = ("dp", "tensor")
BF16 = jnp.bfloat16
F32 = jnp.float32


def number(x, y, z, k):
    return ((z // 2) * 4 + y) * 16 + (z % 2) * 8 + x * 2 + k


CHIPS = [(x, y, z, k) for x in range(4) for y in range(4) for z in range(4) for k in range(2)]


def send(value, dx=0, dy=0, dk=0, zx=0, xx=0, yx=0, zmap=None):
    pairs = []
    for x, y, z, k in CHIPS:
        if zmap is None:
            to = z ^ zx
        elif z in zmap:
            to = zmap[z]
        else:
            continue
        pairs.append(
            (number(x, y, z, k), number(((x + dx) % 4) ^ xx, ((y + dy) % 4) ^ yx, to, k ^ dk))
        )
    return lax.ppermute(value, AXES, pairs)


def nt(a, b):
    return lax.dot_general(a, b, (((1,), (1,)), ((), ())), preferred_element_type=F32)


def place():
    dp, tensor = lax.axis_index("dp"), lax.axis_index("tensor")
    return dp // 4, dp % 4, tensor // 8, (tensor // 2) % 4, tensor % 2


def rotate_kernel(g_ref, cos_ref, sin_ref, swap_ref, x_ref, down_ref, up_ref, y_ref, low_ref):
    cosine = cos_ref[...]
    sine = sin_ref[...]
    odd = (lax.axis_index("tensor") * K_SHARD) % HEAD == K_SHARD
    lane = lax.broadcasted_iota(jnp.int32, cosine.shape, 1)
    key_cos = jnp.where(odd, pltpu.roll(cosine, 64, 1), cosine)
    key_sin = jnp.where(odd, pltpu.roll(sine, 64, 1), sine)
    key_cos = jnp.where(lane < K_SHARD, key_cos, 1.0)
    key_sin = jnp.where(lane < K_SHARD, key_sin, 0.0)
    groups = g_ref.shape[1] // HEAD
    for i in range(groups):
        g = g_ref[:, i * HEAD : (i + 1) * HEAD]
        turned = jnp.dot(g, swap_ref[...], preferred_element_type=F32)
        c = cosine if i < groups - 1 else key_cos
        s = sine if i < groups - 1 else key_sin
        y_ref[:, i * HEAD : (i + 1) * HEAD] = (g.astype(F32) * c + turned * s).astype(BF16)
    low_ref[:RANK, :] = nt(down_ref[...], x_ref[...])
    low_ref[RANK:, :] = nt(up_ref[...], y_ref[...])


def rotate(g, cosine, sine, swap, x, down_t, up):
    rows, width = g.shape
    block = 256
    spec = lambda cols: pl.BlockSpec((block, cols), lambda i: (i, 0))
    whole = lambda a: pl.BlockSpec(a.shape, lambda i: (0, 0))
    return pl.pallas_call(
        rotate_kernel,
        grid=(rows // block,),
        in_specs=[
            spec(width),
            spec(HEAD),
            spec(HEAD),
            whole(swap),
            spec(x.shape[1]),
            whole(down_t),
            whole(up),
        ],
        out_specs=[spec(width), pl.BlockSpec((2 * RANK, block), lambda i: (0, i))],
        out_shape=[
            jax.ShapeDtypeStruct((rows, width), BF16),
            jax.ShapeDtypeStruct((2 * RANK, rows), F32),
        ],
        compiler_params=pltpu.CompilerParams(
            dimension_semantics=("arbitrary",), vmem_limit_bytes=12 << 20
        ),
        cost_estimate=pl.CostEstimate(
            flops=2 * rows * width * 160, bytes_accessed=8 * rows * width, transcendentals=0
        ),
    )(g, cosine, sine, swap, x, down_t, up)


def rows_of(refs, low, high):
    found, start = [], 0
    for ref in refs:
        end = start + ref.shape[0]
        if low < end and high > start:
            found.append(ref[max(low - start, 0) : min(high, end) - start, :])
        start = end
    return found[0] if len(found) == 1 else jnp.concatenate(found, axis=0)


def product_kernel(chunks, keep, start, *refs):
    a_refs, b_refs, pieces = refs[: chunks[0]], refs[chunks[0] : sum(chunks)], refs[sum(chunks) :]
    out_refs = refs[-2:]
    _, y, _, x, k = place()
    core = k if keep else 1 - k
    block = out_refs[0].shape[1]

    def half(of, i, start=0):
        return rows_of(of, start + i * block, start + (i + 1) * block)

    for i in range(2):
        left = jnp.concatenate([half(a_refs, i), half(b_refs, i, start)], axis=1)
        for r in range(4):
            if r == 2:
                kept = jnp.concatenate([pieces[4][core], pieces[5][core]], axis=0)
                other = jnp.concatenate([pieces[6][core], pieces[7][core]], axis=0)
            else:
                first = {0: 0, 1: 2, 3: 8}[r]
                kept, other = pieces[first][core], pieces[first + 1][core]
            total = nt(left, jnp.concatenate([kept, other], axis=1))
            to = (y + r + 4 - x) % 4
            out_refs[i][to] = total.astype(out_refs[i].dtype)


def product(a, b, pieces, keep, start=0):
    rows = sum(c.shape[0] for c in a)
    width = a[0].shape[1]
    cols = pieces[0].shape[1]
    args = [*a, *b, *pieces]
    vmem = pl.BlockSpec(memory_space=pltpu.VMEM)
    return pl.pallas_call(
        functools.partial(product_kernel, (len(a), len(b)), keep, start),
        in_specs=[vmem] * len(args),
        out_specs=[vmem] * 2,
        out_shape=[jax.ShapeDtypeStruct((4, rows // 2, cols), F32 if keep else BF16)] * 2,
        compiler_params=pltpu.CompilerParams(vmem_limit_bytes=16 << 20),
        cost_estimate=pl.CostEstimate(
            flops=2 * rows * 2 * width * 4 * cols,
            bytes_accessed=2 * (2 * rows * width + 8 * cols * width + 4 * rows * cols),
            transcendentals=0,
        ),
    )(*args)


def adapters_kernel(factor, low_ref, more_ref, x_ref, y_ref, low_out, parts_ref):
    low = (low_ref[...] + more_ref[...]).astype(BF16)
    low_out[...] = low
    depth = x_ref.shape[1]
    parts_ref[:, :depth] = factor * jnp.dot(low[RANK:], x_ref[...], preferred_element_type=F32)
    parts_ref[:, depth:] = factor * jnp.dot(low[:RANK], y_ref[...], preferred_element_type=F32)


def adapters(factor, low, more, x, grad_y):
    vmem = pl.BlockSpec(memory_space=pltpu.VMEM)
    cols = x.shape[1] + grad_y.shape[1]
    return pl.pallas_call(
        functools.partial(adapters_kernel, factor),
        in_specs=[vmem] * 4,
        out_specs=[vmem] * 2,
        out_shape=[
            jax.ShapeDtypeStruct(low.shape, BF16),
            jax.ShapeDtypeStruct((RANK, cols), F32),
        ],
        compiler_params=pltpu.CompilerParams(vmem_limit_bytes=12 << 20),
        cost_estimate=pl.CostEstimate(
            flops=16 * RANK * x.shape[0] * cols, bytes_accessed=2 * x.shape[0] * cols, transcendentals=0
        ),
    )(low, more, x, grad_y)


def finish_kernel(
    own_ref, own_moved_ref, far_a, far_b, near_a, near_b, low_ref, down_ref, out_ref
):
    zh, _, zl, _, _ = place()
    stays = zh == zl
    cols = own_ref.shape[1]
    block = 128
    for start in range(0, own_ref.shape[0], block):
        at = slice(start, start + block)
        far = rows_of((far_a, far_b), start, start + block)
        near = rows_of((near_a, near_b), start, start + block)
        first = jnp.where(stays, own_ref[at, :], far)
        second = jnp.where(stays, own_moved_ref[at, :], near)
        adapter = 2.0 * lax.dot_general(
            low_ref[RANK:, at], down_ref[...], (((0,), (0,)), ((), ())), preferred_element_type=F32
        )
        left = jnp.where(zl == 0, first, second)
        right = jnp.where(zl == 0, second, first)
        out_ref[at, :cols] = (left.astype(F32) + adapter[:, :cols]).astype(BF16)
        out_ref[at, cols:] = (right.astype(F32) + adapter[:, cols:]).astype(BF16)


def finish(own, own_moved, far, near, low, down_t):
    rows, cols = own.shape
    vmem = pl.BlockSpec(memory_space=pltpu.VMEM)
    return pl.pallas_call(
        finish_kernel,
        in_specs=[vmem] * 8,
        out_specs=vmem,
        out_shape=jax.ShapeDtypeStruct((rows, 2 * cols), BF16),
        compiler_params=pltpu.CompilerParams(vmem_limit_bytes=12 << 20),
        cost_estimate=pl.CostEstimate(
            flops=64 * rows * cols, bytes_accessed=12 * rows * cols, transcendentals=0
        ),
    )(own, own_moved, *far, *near, low, down_t)


def add_up_kernel(*refs):
    kept, arrived, moved, out_ref = refs[:2], refs[2:4], refs[4:-1], refs[-1]
    rows = kept[0].shape[1]
    for i in range(2):
        at = slice(i * rows, (i + 1) * rows)
        total = kept[i][0] + arrived[i][0].astype(F32)
        if len(moved) == 4:
            total = total + moved[i][...].astype(F32) + moved[2 + i][...].astype(F32)
        else:
            total = total + moved[0][at, :].astype(F32) + moved[1][at, :].astype(F32)
        out_ref[at, :] = total.astype(BF16)


def add_up(kept, arrived, moved):
    _, rows, cols = kept[0].shape
    args = (*kept, *arrived, *moved)
    vmem = pl.BlockSpec(memory_space=pltpu.VMEM)
    return pl.pallas_call(
        add_up_kernel,
        in_specs=[vmem] * len(args),
        out_specs=vmem,
        out_shape=jax.ShapeDtypeStruct((2 * rows, cols), BF16),
        compiler_params=pltpu.CompilerParams(vmem_limit_bytes=14 << 20),
        cost_estimate=pl.CostEstimate(
            flops=8 * rows * cols, bytes_accessed=24 * rows * cols, transcendentals=0
        ),
    )(*args)


def pass_on_kernel(*refs):
    kept, arrived, far_up, far_down, up_ref, down_ref = refs[:2], refs[2:4], *refs[4:]
    rows = kept[0].shape[1]
    for i in range(2):
        at = slice(i * rows, (i + 1) * rows)
        up = kept[i][1] + arrived[i][1].astype(F32)
        down = kept[i][3] + arrived[i][3].astype(F32)
        if i == 0:
            up = up + far_up[...].astype(F32)
        else:
            down = down + far_down[...].astype(F32)
        up_ref[at, :] = up.astype(BF16)
        down_ref[at, :] = down.astype(BF16)


def pass_on(kept, arrived, far_up, far_down):
    _, rows, cols = kept[0].shape
    args = (*kept, *arrived, far_up, far_down)
    vmem = pl.BlockSpec(memory_space=pltpu.VMEM)
    return pl.pallas_call(
        pass_on_kernel,
        in_specs=[vmem] * len(args),
        out_specs=[vmem] * 2,
        out_shape=[jax.ShapeDtypeStruct((2 * rows, cols), BF16)] * 2,
        compiler_params=pltpu.CompilerParams(vmem_limit_bytes=10 << 20),
        cost_estimate=pl.CostEstimate(
            flops=8 * rows * cols, bytes_accessed=24 * rows * cols, transcendentals=0
        ),
    )(*args)


def reduce_in_two(kept, arrived):
    def term(to, low):
        return (kept[low][to] + arrived[low][to].astype(F32)).astype(BF16)

    far_up = send(term(2, False), dx=1)
    far_down = send(term(2, True), dx=-1)
    up, down = pass_on(kept, arrived, far_up, far_down)
    up, down = send(up, dx=1), send(down, dx=-1)
    return add_up(kept, arrived, (up, down))


def in_order(normed_input, positions, weight, down, up, gradient):
    rows, width = gradient.shape
    zl = lax.axis_index("tensor") // 8

    quarters = weight.reshape(2, 2, weight.shape[0] // 4, width)
    kept = lax.dynamic_index_in_dim(quarters, zl, 1, keepdims=False)
    given = lax.dynamic_index_in_dim(quarters, 1 - zl, 1, keepdims=False)
    other = send(given, zx=1)
    half = kept.shape[1] // 2
    k_prev, k_next = send(kept, dy=1), send(kept, dy=-1)
    o_prev, o_next = send(other, dy=1), send(other, dy=-1)
    k_far = send(k_prev[:, :half], dy=1), send(k_next[:, half:], dy=-1)
    o_far = send(o_prev[:, :half], dy=1), send(o_next[:, half:], dy=-1)
    pieces = (kept, other, k_next, o_next, *k_far, *o_far, k_prev, o_prev)

    lanes = jnp.arange(HEAD, dtype=jnp.int32)
    pair = (lanes // 2).astype(F32)
    freq = jnp.float32(500000.0) ** (-2.0 * pair / HEAD)
    angle = positions.astype(F32)[:, None] * freq[None, :]
    row, col = lanes[:, None], lanes[None, :]
    swap = jnp.where(row == (col ^ 1), jnp.where(col % 2 == 0, 1.0, -1.0), 0.0).astype(BF16)
    cosine, sine, down_t = jnp.cos(angle), jnp.sin(angle), down.T
    grad_y, low = rotate(gradient, cosine, sine, swap, normed_input, down_t, up)

    mid = rows // 2
    near_low = send(grad_y[mid:], zx=1)
    near_top = send(grad_y[:mid], zx=1)
    cross = send(grad_y, zx=3)
    far_top = send(cross[:mid], zx=1)
    far_low = send(near_low, zx=3)

    low = low + send(low, zx=1)
    low = low + send(low, dk=1)
    low = low + send(low, xx=1)
    more = send(low, xx=3)
    factor = 2.0 / math.sqrt(rows * 8)
    low, parts = adapters(factor, low, more, normed_input, grad_y)
    parts = parts + send(parts, zx=2)
    parts = parts + send(parts, yx=1)
    parts = parts + send(parts, yx=3)
    grad_a, grad_b = parts[:, : down.shape[0]].T, parts[:, down.shape[0] :]

    sums = []
    for a, b, start in (
        ([grad_y], [near_top, near_low], 0), ([far_low], [cross], mid), ([far_top], [cross], 0)
    ):
        partial = product(a, b, pieces, False, start)
        arrived = [send(p, dk=1) for p in partial]
        total = product(a, b, pieces, True, start)
        sums.append(reduce_in_two(total, arrived))
    own, far_a, far_b = sums

    own_moved = send(own, zmap={1: 0, 2: 3})
    near_a = send(far_a, zx=3)
    far_a = send(near_a, zmap={3: 2, 0: 1})
    near_b = send(far_b, zmap={1: 2, 2: 1})
    far_b = send(far_b, zmap={0: 2, 3: 1})
    grad_x = finish(own, own_moved, (far_b, far_a), (near_b, near_a), low, down_t)
    return grad_x, grad_a, grad_b


def solution(mesh):
    placed = (
        P("dp", "tensor"),
        P("dp"),
        P("dp", "tensor"),
        P("tensor", None),
        P(None, "tensor"),
        P("dp", "tensor"),
    )
    return jax.shard_map(
        in_order,
        mesh=mesh,
        in_specs=placed,
        out_specs=(P("dp", "tensor"), P("tensor", None), P(None, "tensor")),
        check_vma=False,
    )
```
